32 devices in a mesh: dp: 8 (over z, y), rep: 4 (over x, core).
Axes of the slice: x: 2, y: 2, z: 4, core: 2. Of those that a mesh axis runs over, the one named last changes fastest.
Arguments:
- grads: bfloat16 [32, 4096, 512], P(('dp', 'rep')), may hold values from -1000 to 1000
- master: float32 [4096, 512], P('dp'), may hold values from -3 to 3
- first_moment: float32 [4096, 512], P('dp'), may hold values from -2 to 2
- second_moment: float32 [4096, 512], P('dp'), may hold values from 0.01 to 1
Outputs:
- weights: bfloat16 [4096, 512], replicated
- new_master: float32 [4096, 512], P('dp')
- new_first: float32 [4096, 512], P('dp')
- new_second: float32 [4096, 512], P('dp')
The draws below stay inside these ranges and needn't reach their ends.
All inputs are finite; a program needn't handle non-finite values.
Results may differ from the reference program's by a relative error of at most 0.001.
Values may be sent and summed in bfloat16 or wider, within the bound.
A program may use at most 64 MiB of HBM per device.

```python
import math
import jax
import jax.numpy as jnp
from jax import lax

D_WIN = 4096
STEP = 20
COLS = 512
SOURCES = 32
N_REP = 4


def draw_grads(key, part):
    keys = jax.random.split(jax.random.fold_in(key, 11), 3)
    position = jnp.arange(D_WIN, dtype=jnp.float32) / D_WIN
    replica = (jnp.arange(SOURCES, dtype=jnp.int32) % N_REP).astype(jnp.float32) / max(N_REP - 1, 1)
    row_scale = 10.0 ** jax.random.uniform(keys[0], (D_WIN,), jnp.float32) * 5.0 ** position
    col_scale = 10.0 ** jax.random.uniform(keys[1], (COLS,), jnp.float32)
    base = jax.random.normal(keys[2], (SOURCES, D_WIN, COLS), jnp.float32)
    base = base * (1.0 + 2.0 * replica)[:, None, None]
    scaled = base * row_scale[None, :, None] * col_scale[None, None, :]
    return jnp.clip(scaled, -1000.0, 1000.0).astype(jnp.bfloat16)


def block_levels(rng, shape, cuts, low, largest):
    level, own = 1.0, jax.random.fold_in(rng, 6)
    for axis_at, blocks in cuts:
        steps = jnp.exp(jax.random.uniform(jax.random.fold_in(own, axis_at), (blocks,), jnp.float32, low / len(cuts), largest / len(cuts)))
        level = level * jnp.repeat(steps, shape[axis_at] // blocks).reshape([-1 if axis == axis_at else 1 for axis in range(len(shape))])
    return level


def scatter_about(rng, dims, width, limit, cuts=(), held_as=jnp.bfloat16):
    values = width * jax.random.normal(rng, dims, jnp.float32)
    if cuts:
        values = values * block_levels(rng, dims, cuts, -0.22, 0.18)
    return jnp.clip(values, -limit, limit).astype(held_as)


def setup_inputs(seed: int = 0) -> dict:
    splits = jax.random.split(jax.random.key(seed), 5)
    return {
        "grads": draw_grads(jax.random.fold_in(splits[4], 71), 0),
        "master": scatter_about(splits[1], (D_WIN, COLS), 0.5, 3.0, ((0, 8),), jnp.float32),
        "first_moment": scatter_about(splits[2], (D_WIN, COLS), 0.3, 2.0, ((0, 8),), jnp.float32),
        "second_moment": jnp.clip(jnp.exp(math.log(1.0) - 4.6051702 * jax.random.uniform(splits[3], (D_WIN, COLS), jnp.float32) ** block_levels(splits[3], (D_WIN, COLS), ((0, 8),), -0.2, 0.2)), 0.01, 1.0),
    }


def adam_update(clipped, master, first_moment, second_moment):
    new_first = 0.9 * first_moment + 0.1 * clipped
    new_second = 0.95 * second_moment + 0.05 * clipped * clipped
    first_hat = new_first / (1.0 - 0.9 ** STEP)
    second_hat = new_second / (1.0 - 0.95 ** STEP)
    update = first_hat / (jnp.sqrt(second_hat) + 1e-08)
    new_master = master - 0.01 * (update + 0.1 * master)
    return (new_master, new_first, new_second)

def reference(grads, master, first_moment, second_moment):

    def accumulate(index, total):
        piece = lax.dynamic_index_in_dim(grads, index, 0, keepdims=False)
        return total + piece.astype(jnp.float32)
    total = lax.fori_loop(0, SOURCES, accumulate, jnp.zeros((D_WIN, COLS), jnp.float32))
    norm = jnp.sqrt(jnp.sum(total * total))
    threshold = 4.0 * math.sqrt(D_WIN * COLS)
    factor = jnp.minimum(1.0, threshold / (norm + 1e-06))
    new_master, new_first, new_second = adam_update(factor * total, master, first_moment, second_moment)
    return (new_master.astype(jnp.bfloat16), new_master, new_first, new_second)
```

```python
import functools
import math

import jax
import jax.numpy as jnp
from jax import lax
from jax.experimental import pallas as pl
from jax.experimental.pallas import tpu as pltpu
from jax.sharding import PartitionSpec as P

STEP = 20
MESH = pl.DeviceIdType.MESH
F32 = jnp.float32


def adam_update(clipped, master, first_moment, second_moment):
    new_first = 0.9 * first_moment + 0.1 * clipped
    new_second = 0.95 * second_moment + 0.05 * clipped * clipped
    first_hat = new_first / (1.0 - 0.9**STEP)
    second_hat = new_second / (1.0 - 0.95**STEP)
    update = first_hat / (jnp.sqrt(second_hat) + 1e-08)
    new_master = master - 0.01 * (update + 0.1 * master)
    return (new_master, new_first, new_second)


def clip_factor(squares, entries):
    threshold = 4.0 * math.sqrt(entries)
    return jnp.minimum(1.0, threshold / (jnp.sqrt(squares) + 1e-06))


def kernel(
    Z, R, entries,
    g, m_in, f_in, s_in,
    w_out, m_out, f_out, s_out,
    mine, swapped, S, RA, RB, R2, R3, V, N, M, F, Q, W,
    load_sem, state_sem, out_sem, wout_sem,
    g_sem, a1_sem, b1_sem, a2_sem, b2_sem, z_sem, n_sem, v_sem,
    gz_sem, ga_sem, gb_sem, ha_sem, hb_sem, gc_sem,
):
    D = 2 * Z
    n = D * R
    d, r = lax.axis_index("dp"), lax.axis_index("rep")
    z, y = d // 2, d % 2
    x, c = r // 2, r % 2
    me = d * R + r
    to_x = (d, (1 - x) * 2 + c)
    to_y = (z * 2 + 1 - y, r)
    to_c = (d, x * 2 + 1 - c)

    def to_z(other):
        return (other * 2 + y, r)

    def push(src, dst, sems, index, device):
        return pltpu.make_async_remote_copy(
            src_ref=src, dst_ref=dst, send_sem=sems.at[(0,) + index], recv_sem=sems.at[(1,) + index],
            device_id=device, device_id_type=MESH,
        )

    def dest(k):
        return (z + 1 + k) % Z

    barrier = pltpu.get_barrier_semaphore()

    @pl.loop(1, n)
    def _(k):
        t = (me + k) % n
        pl.semaphore_signal(barrier, inc=1, device_id=(t // R, t % R), device_id_type=MESH)

    def load(k):
        return pltpu.make_async_copy(g.at[dest(k), :, c], mine.at[k], load_sem.at[k])

    @pl.loop(0, Z)
    def _(k):
        load(k).start()

    states = [
        pltpu.make_async_copy(a, b, state_sem.at[i])
        for i, (a, b) in enumerate([(m_in, M), (f_in, F), (s_in, Q)])
    ]
    for copy in states:
        copy.start()
    pl.semaphore_wait(barrier, n - 1)

    def swap(k):
        return push(g.at[dest(k), :, 1 - c], swapped.at[k], g_sem, (k,), to_c)

    @pl.loop(0, Z)
    def _(k):
        swap(k).start()

    def first_a(k):
        return push(S.at[k, :, 1 - x, 0], RA.at[k], a1_sem, (k,), to_x)

    def first_b(k):
        return push(S.at[k, 1 - y, :, 1], RB.at[k], b1_sem, (k,), to_y)

    def second_a(k):
        return push(S.at[k, 1 - y, x, 0], R2.at[k, 0], a2_sem, (k,), to_y)

    def second_b(k):
        return push(S.at[k, y, 1 - x, 1], R2.at[k, 1], b2_sem, (k,), to_x)

    def along_z(k):
        return push(S.at[k, y, x], R3.at[k], z_sem, (k,), to_z(dest(k)))

    @pl.loop(0, Z + 2)
    def _(step):
        @pl.when(step < Z)
        def _():
            k = step
            load(k).wait()
            swap(k).wait_recv()
            S[k] = mine[k].astype(F32) + swapped[k].astype(F32)
            first_a(k).start()
            first_b(k).start()

        @pl.when((step >= 1) & (step < Z + 1))
        def _():
            k = step - 1
            first_a(k).wait_recv()
            S[k, :, x, 0] = S[k, :, x, 0] + RA[k]
            second_a(k).start()
            first_b(k).wait_recv()
            S[k, y, :, 1] = S[k, y, :, 1] + RB[k]
            second_b(k).start()

        @pl.when(step >= 2)
        def _():
            k = step - 2
            second_a(k).wait_recv()
            second_b(k).wait_recv()
            S[k, y, x] = S[k, y, x] + R2[k]

            @pl.when(k < Z - 1)
            def _():
                along_z(k).start()

    @pl.loop(0, Z - 1)
    def _(k):
        along_z(k).wait_recv()
        S[Z - 1, y, x] = S[Z - 1, y, x] + R3[k]

    total = S[Z - 1, y, x]
    V[c, x] = total
    lanes = jnp.sum((total * total).reshape(-1, total.shape[-1]), axis=0, keepdims=True)
    N[me] = sum(lanes[:, i : i + 128] for i in range(0, total.shape[-1], 128))

    def norm_part(k):
        t = (me + k) % n
        return push(N.at[me], N.at[me], n_sem, (k,), (t // R, t % R))

    def norm_recv(k):
        t = (me + n - k) % n
        return push(N.at[t], N.at[t], n_sem, (k,), (t // R, t % R))

    @pl.loop(1, n)
    def _(k):
        norm_part(k).start()

    v_x = push(V.at[c, x], V.at[c, x], v_sem, (0,), to_x)
    v_c = push(V.at[c, x], V.at[c, x], v_sem, (1,), to_c)
    v_xc = push(V.at[c, 1 - x], V.at[c, 1 - x], v_sem, (2,), to_c)
    got_x = push(V.at[c, 1 - x], V.at[c, 1 - x], v_sem, (0,), to_x)
    got_c = push(V.at[1 - c, x], V.at[1 - c, x], v_sem, (1,), to_c)
    got_xc = push(V.at[1 - c, 1 - x], V.at[1 - c, 1 - x], v_sem, (2,), to_c)
    v_x.start()
    v_c.start()

    for copy in states:
        copy.wait()

    @pl.loop(1, n)
    def _(k):
        norm_recv(k).wait_recv()

    factor = clip_factor(jnp.sum(N[...]), entries)

    def update(cc, xx):
        new_master, new_first, new_second = adam_update(factor * V[cc, xx], M[cc, xx], F[cc, xx], Q[cc, xx])
        M[cc, xx] = new_master
        F[cc, xx] = new_first
        Q[cc, xx] = new_second
        return new_master

    W[z, y, c, x] = update(c, x).astype(jnp.bfloat16)

    def source(b):
        return (z + Z - b) % Z

    def gather_z(j):
        return push(W.at[z, y, c, x], W.at[z, y, c, x], gz_sem, (j,), to_z(dest(j)))

    def got_z(j):
        block = W.at[source(j + 1), y, c, x]
        return push(block, block, gz_sem, (j,), to_z(dest(j)))

    @pl.loop(0, Z - 1)
    def _(j):
        gather_z(j).start()

    def same(ref, sems, b, device):
        return push(ref, ref, sems, (b,), device)

    def ga(b, yy):
        return same(W.at[source(b), yy, c, x, 0], ga_sem, b, to_y)

    def gb(b, xx):
        return same(W.at[source(b), y, c, xx, 1], gb_sem, b, to_x)

    def ha(b, xx):
        return same(W.at[source(b), :, c, xx, 0], ha_sem, b, to_x)

    def hb(b, yy):
        return same(W.at[source(b), yy, c, :, 1], hb_sem, b, to_y)

    def gc(b, cc):
        return same(W.at[source(b), :, cc], gc_sem, b, to_c)

    def w_copy(b):
        return pltpu.make_async_copy(W.at[source(b)], w_out.at[source(b)], wout_sem.at[b])

    @pl.loop(0, Z + 3)
    def _(step):
        @pl.when(step < Z)
        def _():
            b = step

            @pl.when(b >= 1)
            def _():
                got_z(b - 1).wait_recv()

            ga(b, y).start()
            gb(b, x).start()

        @pl.when((step >= 1) & (step < Z + 1))
        def _():
            b = step - 1
            ga(b, 1 - y).wait_recv()
            ha(b, x).start()
            gb(b, 1 - x).wait_recv()
            hb(b, y).start()

        @pl.when(step == 1)
        def _():
            got_x.wait_recv()
            v_xc.start()
            update(c, 1 - x)
            got_c.wait_recv()
            update(1 - c, x)
            got_xc.wait_recv()
            update(1 - c, 1 - x)
            for i, (a, b) in enumerate([(M, m_out), (F, f_out), (Q, s_out)]):
                pltpu.make_async_copy(a, b, out_sem.at[i]).start()

        @pl.when((step >= 2) & (step < Z + 2))
        def _():
            b = step - 2
            ha(b, 1 - x).wait_recv()
            hb(b, 1 - y).wait_recv()
            gc(b, c).start()

        @pl.when(step >= 3)
        def _():
            b = step - 3
            gc(b, 1 - c).wait_recv()
            w_copy(b).start()

    for i, (a, b) in enumerate([(M, m_out), (F, f_out), (Q, s_out)]):
        pltpu.make_async_copy(a, b, out_sem.at[i]).wait()
    v_x.wait_send()
    v_c.wait_send()
    v_xc.wait_send()

    @pl.loop(1, n)
    def _(k):
        norm_part(k).wait_send()

    @pl.loop(0, Z)
    def _(k):
        swap(k).wait_send()
        first_a(k).wait_send()
        first_b(k).wait_send()
        second_a(k).wait_send()
        second_b(k).wait_send()
        ga(k, y).wait_send()
        gb(k, x).wait_send()
        ha(k, x).wait_send()
        hb(k, y).wait_send()
        gc(k, c).wait_send()
        w_copy(k).wait()

    @pl.loop(0, Z - 1)
    def _(k):
        along_z(k).wait_send()
        gather_z(k).wait_send()


def body(D, R, grads, master, first_moment, second_moment):
    rows, cols = grads.shape[1:]
    Z, n = D // 2, D * R
    t = rows // (D * R * 2)
    any_space = pl.BlockSpec(memory_space=pl.ANY)
    bf16 = jnp.bfloat16
    part = (2, 2, 2, t, cols)
    dma = pltpu.SemaphoreType.DMA
    state = jax.ShapeDtypeStruct(part, F32)
    outs = pl.pallas_call(
        functools.partial(kernel, Z, R, rows * cols),
        out_shape=[jax.ShapeDtypeStruct((Z, 2) + part, bf16), state, state, state],
        in_specs=[any_space] * 4,
        out_specs=[any_space] * 4,
        scratch_shapes=[
            pltpu.VMEM((Z,) + part, bf16),
            pltpu.VMEM((Z,) + part, bf16),
            pltpu.VMEM((Z,) + part, F32),
            pltpu.VMEM((Z, 2, t, cols), F32),
            pltpu.VMEM((Z, 2, t, cols), F32),
            pltpu.VMEM((Z, 2, t, cols), F32),
            pltpu.VMEM((Z - 1, 2, t, cols), F32),
            pltpu.VMEM(part, F32),
            pltpu.VMEM((n, 1, 128), F32),
            pltpu.VMEM(part, F32),
            pltpu.VMEM(part, F32),
            pltpu.VMEM(part, F32),
            pltpu.VMEM((Z, 2) + part, bf16),
            dma((Z,)), dma((3,)), dma((3,)), dma((Z,)),
            dma((2, Z)), dma((2, Z)), dma((2, Z)), dma((2, Z)), dma((2, Z)), dma((2, Z)),
            dma((2, n)), dma((2, 3)),
            dma((2, Z)), dma((2, Z)), dma((2, Z)), dma((2, Z)), dma((2, Z)), dma((2, Z)),
        ],
        compiler_params=pltpu.CompilerParams(
            collective_id=0, has_side_effects=True, vmem_limit_bytes=48 * 1024 * 1024
        ),
    )(
        grads.reshape((Z, 2) + part),
        master.reshape(part), first_moment.reshape(part), second_moment.reshape(part),
    )
    weights, new_master, new_first, new_second = outs
    block = (rows // D, cols)
    return (weights.reshape(rows, cols), new_master.reshape(block), new_first.reshape(block), new_second.reshape(block))


def solution(mesh):
    D, R = mesh.shape["dp"], mesh.shape["rep"]
    assert R == 4 and D % 2 == 0
    in_specs = (P(("dp", "rep"), None, None), P("dp", None), P("dp", None), P("dp", None))
    out_specs = (P(), P("dp", None), P("dp", None), P("dp", None))
    return jax.shard_map(
        functools.partial(body, D, R), mesh=mesh, in_specs=in_specs, out_specs=out_specs, check_vma=False
    )
```

```python
import functools
import math

import jax
import jax.numpy as jnp
from jax import lax
from jax.experimental import pallas as pl
from jax.experimental.pallas import tpu as pltpu
from jax.sharding import PartitionSpec as P

STEP = 20
MESH = pl.DeviceIdType.MESH
F32 = jnp.float32
VMEM_BYTES = 63 * 1024 * 1024


def adam_update(clipped, master, first_moment, second_moment):
    new_first = 0.9 * first_moment + 0.1 * clipped
    new_second = 0.95 * second_moment + 0.05 * clipped * clipped
    first_hat = new_first / (1.0 - 0.9**STEP)
    second_hat = new_second / (1.0 - 0.95**STEP)
    update = first_hat / (jnp.sqrt(second_hat) + 1e-08)
    new_master = master - 0.01 * (update + 0.1 * master)
    return (new_master, new_first, new_second)


def clip_factor(squares, entries):
    threshold = 4.0 * math.sqrt(entries)
    return jnp.minimum(1.0, threshold / (jnp.sqrt(squares) + 1e-06))


def kernel(
    Z, R, entries,
    g, m_in, f_in, s_in,
    W, M, F, Q,
    mine, swapped, S, RA, RB, R2, R3, V, N,
    load_sem, state_sem,
    g_sem, a1_sem, b1_sem, a2_sem, b2_sem, z_sem, n_sem, v_sem,
    gz_sem, ga_sem, gb_sem, ha_sem, hb_sem, gc_sem,
):
    D = 2 * Z
    n = D * R
    d, r = lax.axis_index("dp"), lax.axis_index("rep")
    z, y = d // 2, d % 2
    x, c = r // 2, r % 2
    me = d * R + r
    to_x = (d, (1 - x) * 2 + c)
    to_y = (z * 2 + 1 - y, r)
    to_c = (d, x * 2 + 1 - c)

    def to_z(other):
        return (other * 2 + y, r)

    def push(src, dst, sems, index, device):
        return pltpu.make_async_remote_copy(
            src_ref=src, dst_ref=dst, send_sem=sems.at[(0,) + index], recv_sem=sems.at[(1,) + index],
            device_id=device, device_id_type=MESH,
        )

    def dest(k):
        return (z + 1 + k) % Z

    barrier = pltpu.get_barrier_semaphore()

    @pl.loop(1, n)
    def _(k):
        t = (me + k) % n
        pl.semaphore_signal(barrier, inc=1, device_id=(t // R, t % R), device_id_type=MESH)

    def load(k):
        return pltpu.make_async_copy(g.at[dest(k), :, c], mine.at[k], load_sem.at[k])

    @pl.loop(0, Z)
    def _(k):
        load(k).start()

    states = [
        pltpu.make_async_copy(a, b, state_sem.at[i])
        for i, (a, b) in enumerate([(m_in, M), (f_in, F), (s_in, Q)])
    ]
    for copy in states:
        copy.start()
    pl.semaphore_wait(barrier, n - 1)

    def swap(k):
        return push(g.at[dest(k), :, 1 - c], swapped.at[k], g_sem, (k,), to_c)

    @pl.loop(0, Z)
    def _(k):
        swap(k).start()

    def first_a(k):
        return push(S.at[k, :, 1 - x, 0], RA.at[k], a1_sem, (k,), to_x)

    def first_b(k):
        return push(S.at[k, 1 - y, :, 1], RB.at[k], b1_sem, (k,), to_y)

    def second_a(k):
        return push(S.at[k, 1 - y, x, 0], R2.at[k, 0], a2_sem, (k,), to_y)

    def second_b(k):
        return push(S.at[k, y, 1 - x, 1], R2.at[k, 1], b2_sem, (k,), to_x)

    def along_z(k):
        return push(S.at[k, y, x], R3.at[k], z_sem, (k,), to_z(dest(k)))

    @pl.loop(0, Z + 2)
    def _(step):
        @pl.when(step < Z)
        def _():
            k = step
            load(k).wait()
            swap(k).wait_recv()
            S[k] = mine[k].astype(F32) + swapped[k].astype(F32)
            first_a(k).start()
            first_b(k).start()

        @pl.when((step >= 1) & (step < Z + 1))
        def _():
            k = step - 1
            first_a(k).wait_recv()
            S[k, :, x, 0] = S[k, :, x, 0] + RA[k]
            second_a(k).start()
            first_b(k).wait_recv()
            S[k, y, :, 1] = S[k, y, :, 1] + RB[k]
            second_b(k).start()

        @pl.when(step >= 2)
        def _():
            k = step - 2
            second_a(k).wait_recv()
            second_b(k).wait_recv()
            S[k, y, x] = S[k, y, x] + R2[k]

            @pl.when(k < Z - 1)
            def _():
                along_z(k).start()

    @pl.loop(0, Z - 1)
    def _(k):
        along_z(k).wait_recv()
        S[Z - 1, y, x] = S[Z - 1, y, x] + R3[k]

    total = S[Z - 1, y, x]
    V[c, x] = total
    lanes = jnp.sum((total * total).reshape(-1, total.shape[-1]), axis=0, keepdims=True)
    N[me] = sum(lanes[:, i : i + 128] for i in range(0, total.shape[-1], 128))

    def norm_part(k):
        t = (me + k) % n
        return push(N.at[me], N.at[me], n_sem, (k,), (t // R, t % R))

    def norm_recv(k):
        t = (me + n - k) % n
        return push(N.at[t], N.at[t], n_sem, (k,), (t // R, t % R))

    @pl.loop(1, n)
    def _(k):
        norm_part(k).start()

    v_x = push(V.at[c, x], V.at[c, x], v_sem, (0,), to_x)
    v_c = push(V.at[c, x], V.at[c, x], v_sem, (1,), to_c)
    v_xc = push(V.at[c, 1 - x], V.at[c, 1 - x], v_sem, (2,), to_c)
    got_x = push(V.at[c, 1 - x], V.at[c, 1 - x], v_sem, (0,), to_x)
    got_c = push(V.at[1 - c, x], V.at[1 - c, x], v_sem, (1,), to_c)
    got_xc = push(V.at[1 - c, 1 - x], V.at[1 - c, 1 - x], v_sem, (2,), to_c)
    v_x.start()
    v_c.start()

    for copy in states:
        copy.wait()

    @pl.loop(1, n)
    def _(k):
        norm_recv(k).wait_recv()

    factor = clip_factor(jnp.sum(N[...]), entries)

    def update(cc, xx):
        new_master, new_first, new_second = adam_update(factor * V[cc, xx], M[cc, xx], F[cc, xx], Q[cc, xx])
        M[cc, xx] = new_master
        F[cc, xx] = new_first
        Q[cc, xx] = new_second
        return new_master

    W[z, y, c, x] = update(c, x).astype(jnp.bfloat16)

    def source(b):
        return (z + Z - b) % Z

    def gather_z(j):
        return push(W.at[z, y, c, x], W.at[z, y, c, x], gz_sem, (j,), to_z(dest(j)))

    def got_z(j):
        block = W.at[source(j + 1), y, c, x]
        return push(block, block, gz_sem, (j,), to_z(dest(j)))

    @pl.loop(0, Z - 1)
    def _(j):
        gather_z(j).start()

    def same(ref, sems, b, device):
        return push(ref, ref, sems, (b,), device)

    def ga(b, yy):
        return same(W.at[source(b), yy, c, x, 0], ga_sem, b, to_y)

    def gb(b, xx):
        return same(W.at[source(b), y, c, xx, 1], gb_sem, b, to_x)

    def ha(b, xx):
        return same(W.at[source(b), :, c, xx, 0], ha_sem, b, to_x)

    def hb(b, yy):
        return same(W.at[source(b), yy, c, :, 1], hb_sem, b, to_y)

    def gc(b, cc):
        return same(W.at[source(b), :, cc], gc_sem, b, to_c)

    @pl.loop(0, Z + 2)
    def _(step):
        @pl.when((step >= 1) & (step < Z + 1))
        def _():
            b = step - 1
            ga(b, 1 - y).wait_recv()
            ha(b, x).start()
            gb(b, 1 - x).wait_recv()
            hb(b, y).start()

        @pl.when(step < Z)
        def _():
            b = step

            @pl.when(b >= 1)
            def _():
                got_z(b - 1).wait_recv()

            ga(b, y).start()
            gb(b, x).start()

        @pl.when(step == 1)
        def _():
            got_x.wait_recv()
            v_xc.start()
            update(c, 1 - x)
            got_c.wait_recv()
            update(1 - c, x)
            got_xc.wait_recv()
            update(1 - c, 1 - x)

        @pl.when(step >= 2)
        def _():
            b = step - 2
            ha(b, 1 - x).wait_recv()
            hb(b, 1 - y).wait_recv()
            gc(b, c).start()

    @pl.loop(0, Z)
    def _(b):
        gc(b, 1 - c).wait_recv()

    v_x.wait_send()
    v_c.wait_send()
    v_xc.wait_send()

    @pl.loop(1, n)
    def _(k):
        norm_part(k).wait_send()

    @pl.loop(0, Z)
    def _(k):
        swap(k).wait_send()
        first_a(k).wait_send()
        first_b(k).wait_send()
        second_a(k).wait_send()
        second_b(k).wait_send()
        ga(k, y).wait_send()
        gb(k, x).wait_send()
        ha(k, x).wait_send()
        hb(k, y).wait_send()
        gc(k, c).wait_send()

    @pl.loop(0, Z - 1)
    def _(k):
        along_z(k).wait_send()
        gather_z(k).wait_send()


def write_out(*refs):
    srcs, dsts, sems = refs[:4], refs[4:8], refs[8]
    copies = [pltpu.make_async_copy(a, b, sems.at[i]) for i, (a, b) in enumerate(zip(srcs, dsts))]
    for copy in copies:
        copy.start()
    for copy in copies:
        copy.wait()


def body(D, R, grads, master, first_moment, second_moment):
    rows, cols = grads.shape[1:]
    Z, n = D // 2, D * R
    t = rows // (D * R * 2)
    hbm = pl.BlockSpec(memory_space=pltpu.HBM)
    vmem = pl.BlockSpec(memory_space=pltpu.VMEM)
    bf16 = jnp.bfloat16
    part = (2, 2, 2, t, cols)
    dma = pltpu.SemaphoreType.DMA
    shapes = [((Z, 2) + part, bf16)] + [(part, F32)] * 3
    held_bytes = sum(math.prod(dims) * jnp.dtype(kind).itemsize for dims, kind in shapes)
    held = pl.pallas_call(
        functools.partial(kernel, Z, R, rows * cols),
        out_shape=[pltpu.VMEM(*shape) for shape in shapes],
        in_specs=[hbm] * 4,
        out_specs=[vmem] * 4,
        scratch_shapes=[
            pltpu.VMEM((Z,) + part, bf16),
            pltpu.VMEM((Z,) + part, bf16),
            pltpu.VMEM((Z,) + part, F32),
            pltpu.VMEM((Z, 2, t, cols), F32),
            pltpu.VMEM((Z, 2, t, cols), F32),
            pltpu.VMEM((Z, 2, t, cols), F32),
            pltpu.VMEM((Z - 1, 2, t, cols), F32),
            pltpu.VMEM(part, F32),
            pltpu.VMEM((n, 1, 128), F32),
            dma((Z,)), dma((3,)),
            dma((2, Z)), dma((2, Z)), dma((2, Z)), dma((2, Z)), dma((2, Z)), dma((2, Z)),
            dma((2, n)), dma((2, 3)),
            dma((2, Z)), dma((2, Z)), dma((2, Z)), dma((2, Z)), dma((2, Z)), dma((2, Z)),
        ],
        compiler_params=pltpu.CompilerParams(
            collective_id=0, has_side_effects=True, vmem_limit_bytes=VMEM_BYTES - held_bytes
        ),
    )(
        grads.reshape((Z, 2) + part),
        master.reshape(part), first_moment.reshape(part), second_moment.reshape(part),
    )
    outs = pl.pallas_call(
        write_out,
        out_shape=[jax.ShapeDtypeStruct(*shape) for shape in shapes],
        in_specs=[vmem] * 4,
        out_specs=[hbm] * 4,
        scratch_shapes=[dma((4,))],
        compiler_params=pltpu.CompilerParams(vmem_limit_bytes=1024 * 1024),
    )(*held)
    weights, new_master, new_first, new_second = outs
    block = (rows // D, cols)
    return (weights.reshape(rows, cols), new_master.reshape(block), new_first.reshape(block), new_second.reshape(block))


def solution(mesh):
    D, R = mesh.shape["dp"], mesh.shape["rep"]
    assert R == 4 and D % 2 == 0
    in_specs = (P(("dp", "rep"), None, None), P("dp", None), P("dp", None), P("dp", None))
    out_specs = (P(), P("dp", None), P("dp", None), P("dp", None))
    return jax.shard_map(
        functools.partial(body, D, R), mesh=mesh, in_specs=in_specs, out_specs=out_specs, check_vma=False
    )
```

```python
import functools
import math

import jax
import jax.numpy as jnp
from jax import lax
from jax.experimental import pallas as pl
from jax.experimental.pallas import tpu as pltpu
from jax.sharding import PartitionSpec as P

STEP = 20
MESH = pl.DeviceIdType.MESH
F32 = jnp.float32
VMEM_BYTES = 63 * 1024 * 1024


def adam_update(clipped, master, first_moment, second_moment):
    new_first = 0.9 * first_moment + 0.1 * clipped
    new_second = 0.95 * second_moment + 0.05 * clipped * clipped
    first_hat = new_first / (1.0 - 0.9**STEP)
    second_hat = new_second / (1.0 - 0.95**STEP)
    update = first_hat / (jnp.sqrt(second_hat) + 1e-08)
    new_master = master - 0.01 * (update + 0.1 * master)
    return (new_master, new_first, new_second)


def clip_factor(squares, entries):
    threshold = 4.0 * math.sqrt(entries)
    return jnp.minimum(1.0, threshold / (jnp.sqrt(squares) + 1e-06))


def kernel(
    Z, R, entries,
    g, m_in, f_in, s_in,
    W, M, F, Q,
    mine, swapped, S, RA, RB, R2, R3, V, N,
    load_sem, state_sem,
    g_sem, a1_sem, b1_sem, a2_sem, b2_sem, z_sem, n_sem, v_sem,
    gz_sem, ga_sem, gb_sem, ha_sem, hb_sem, gc_sem,
):
    D = 2 * Z
    n = D * R
    d, r = lax.axis_index("dp"), lax.axis_index("rep")
    z, y = d // 2, d % 2
    x, c = r // 2, r % 2
    me = d * R + r
    half = g.shape[-1] // 2
    C = 2 * Z
    to_x = (d, (1 - x) * 2 + c)
    to_y = (z * 2 + 1 - y, r)
    to_c = (d, x * 2 + 1 - c)

    def to_z(other):
        return (other * 2 + y, r)

    def push(src, dst, sems, index, device):
        return pltpu.make_async_remote_copy(
            src_ref=src, dst_ref=dst, send_sem=sems.at[(0,) + index], recv_sem=sems.at[(1,) + index],
            device_id=device, device_id_type=MESH,
        )

    def dest(k):
        return (z + 1 + k) % Z

    def cols(q):
        return pl.ds(pl.multiple_of((q % 2) * half, half), half)

    barrier = pltpu.get_barrier_semaphore()

    @pl.loop(1, n)
    def _(k):
        t = (me + k) % n
        pl.semaphore_signal(barrier, inc=1, device_id=(t // R, t % R), device_id_type=MESH)

    def load(k):
        return pltpu.make_async_copy(
            g.at[dest(k // 2), :, c, :, :, :, cols(k)], mine.at[k // 2, :, :, :, :, cols(k)], load_sem.at[k]
        )

    @pl.loop(0, C)
    def _(k):
        load(k).start()

    states = [
        pltpu.make_async_copy(a, b, state_sem.at[i])
        for i, (a, b) in enumerate([(m_in, M), (f_in, F), (s_in, Q)])
    ]
    for copy in states:
        copy.start()
    pl.semaphore_wait(barrier, n - 1)

    def swap(k):
        return push(
            g.at[dest(k // 2), :, 1 - c, :, :, :, cols(k)], swapped.at[k // 2, :, :, :, :, cols(k)],
            g_sem, (k,), to_c,
        )

    @pl.loop(0, C)
    def _(k):
        swap(k).start()

    def first_a(k):
        i, p = k // 2, cols(k)
        return push(S.at[i, :, 1 - x, 0, :, p], RA.at[i, :, :, p], a1_sem, (k,), to_x)

    def first_b(k):
        i, p = k // 2, cols(k)
        return push(S.at[i, 1 - y, :, 1, :, p], RB.at[i, :, :, p], b1_sem, (k,), to_y)

    def second_a(k):
        i, p = k // 2, cols(k)
        return push(S.at[i, 1 - y, x, 0, :, p], R2.at[i, 0, :, p], a2_sem, (k,), to_y)

    def second_b(k):
        i, p = k // 2, cols(k)
        return push(S.at[i, y, 1 - x, 1, :, p], R2.at[i, 1, :, p], b2_sem, (k,), to_x)

    def along_z(k):
        i, p = k // 2, cols(k)
        return push(S.at[i, y, x, :, :, p], R3.at[i, :, :, p], z_sem, (k,), to_z(dest(i)))

    @pl.loop(0, C + 2)
    def _(step):
        @pl.when(step < C)
        def _():
            k = step
            i, p = k // 2, cols(k)
            load(k).wait()
            swap(k).wait_recv()
            S[i, :, :, :, :, p] = mine[i, :, :, :, :, p].astype(F32) + swapped[i, :, :, :, :, p].astype(F32)
            first_a(k).start()
            first_b(k).start()

        @pl.when((step >= 1) & (step < C + 1))
        def _():
            k = step - 1
            i, p = k // 2, cols(k)
            first_a(k).wait_recv()
            S[i, :, x, 0, :, p] = S[i, :, x, 0, :, p] + RA[i, :, :, p]
            second_a(k).start()
            first_b(k).wait_recv()
            S[i, y, :, 1, :, p] = S[i, y, :, 1, :, p] + RB[i, :, :, p]
            second_b(k).start()

        @pl.when(step >= 2)
        def _():
            k = step - 2
            i, p = k // 2, cols(k)
            second_a(k).wait_recv()
            second_b(k).wait_recv()
            S[i, y, x, :, :, p] = S[i, y, x, :, :, p] + R2[i, :, :, p]

            @pl.when(k < C - 2)
            def _():
                along_z(k).start()

    @pl.loop(0, C - 2)
    def _(k):
        i, p = k // 2, cols(k)
        along_z(k).wait_recv()
        S[Z - 1, y, x, :, :, p] = S[Z - 1, y, x, :, :, p] + R3[i, :, :, p]

    total = S[Z - 1, y, x]
    V[c, x] = total
    lanes = jnp.sum((total * total).reshape(-1, total.shape[-1]), axis=0, keepdims=True)
    N[me] = sum(lanes[:, i : i + 128] for i in range(0, total.shape[-1], 128))

    def norm_part(k):
        t = (me + k) % n
        return push(N.at[me], N.at[me], n_sem, (k,), (t // R, t % R))

    def norm_recv(k):
        t = (me + n - k) % n
        return push(N.at[t], N.at[t], n_sem, (k,), (t // R, t % R))

    @pl.loop(1, n)
    def _(k):
        norm_part(k).start()

    v_x = push(V.at[c, x], V.at[c, x], v_sem, (0,), to_x)
    v_c = push(V.at[c, x], V.at[c, x], v_sem, (1,), to_c)
    v_xc = push(V.at[c, 1 - x], V.at[c, 1 - x], v_sem, (2,), to_c)
    got_x = push(V.at[c, 1 - x], V.at[c, 1 - x], v_sem, (0,), to_x)
    got_c = push(V.at[1 - c, x], V.at[1 - c, x], v_sem, (1,), to_c)
    got_xc = push(V.at[1 - c, 1 - x], V.at[1 - c, 1 - x], v_sem, (2,), to_c)
    v_x.start()
    v_c.start()

    for copy in states:
        copy.wait()

    @pl.loop(1, n)
    def _(k):
        norm_recv(k).wait_recv()

    factor = clip_factor(jnp.sum(N[...]), entries)

    def update(cc, xx):
        new_master, new_first, new_second = adam_update(factor * V[cc, xx], M[cc, xx], F[cc, xx], Q[cc, xx])
        M[cc, xx] = new_master
        F[cc, xx] = new_first
        Q[cc, xx] = new_second
        return new_master

    W[z, y, c, x] = update(c, x).astype(jnp.bfloat16)

    def source(b):
        return (z + Z - b // 2) % Z

    def gather_z(j):
        block = W.at[z, y, c, x, :, :, cols(j)]
        return push(block, block, gz_sem, (j,), to_z(dest(j // 2)))

    def got_z(j):
        block = W.at[source(j + 2), y, c, x, :, :, cols(j)]
        return push(block, block, gz_sem, (j,), to_z(dest(j // 2)))

    @pl.loop(0, C - 2)
    def _(j):
        gather_z(j).start()

    def same(ref, sems, b, device):
        return push(ref, ref, sems, (b,), device)

    def ga(b, yy):
        return same(W.at[source(b), yy, c, x, 0, :, cols(b)], ga_sem, b, to_y)

    def gb(b, xx):
        return same(W.at[source(b), y, c, xx, 1, :, cols(b)], gb_sem, b, to_x)

    def ha(b, xx):
        return same(W.at[source(b), :, c, xx, 0, :, cols(b)], ha_sem, b, to_x)

    def hb(b, yy):
        return same(W.at[source(b), yy, c, :, 1, :, cols(b)], hb_sem, b, to_y)

    def gc(b, cc):
        return same(W.at[source(b), :, cc, :, :, :, cols(b)], gc_sem, b, to_c)

    @pl.loop(0, C + 2)
    def _(step):
        @pl.when((step >= 1) & (step < C + 1))
        def _():
            b = step - 1
            ga(b, 1 - y).wait_recv()
            ha(b, x).start()
            gb(b, 1 - x).wait_recv()
            hb(b, y).start()

        @pl.when(step < C)
        def _():
            b = step

            @pl.when(b >= 2)
            def _():
                got_z(b - 2).wait_recv()

            ga(b, y).start()
            gb(b, x).start()

        @pl.when(step == 1)
        def _():
            got_x.wait_recv()
            v_xc.start()
            update(c, 1 - x)

        @pl.when(step == 2)
        def _():
            got_c.wait_recv()
            update(1 - c, x)

        @pl.when(step == 3)
        def _():
            got_xc.wait_recv()
            update(1 - c, 1 - x)

        @pl.when(step >= 2)
        def _():
            b = step - 2
            ha(b, 1 - x).wait_recv()
            hb(b, 1 - y).wait_recv()
            gc(b, c).start()

    @pl.loop(0, C)
    def _(b):
        gc(b, 1 - c).wait_recv()

    v_x.wait_send()
    v_c.wait_send()
    v_xc.wait_send()

    @pl.loop(1, n)
    def _(k):
        norm_part(k).wait_send()

    @pl.loop(0, C)
    def _(k):
        swap(k).wait_send()
        first_a(k).wait_send()
        first_b(k).wait_send()
        second_a(k).wait_send()
        second_b(k).wait_send()
        ga(k, y).wait_send()
        gb(k, x).wait_send()
        ha(k, x).wait_send()
        hb(k, y).wait_send()
        gc(k, c).wait_send()

    @pl.loop(0, C - 2)
    def _(k):
        along_z(k).wait_send()
        gather_z(k).wait_send()


def write_out(*refs):
    srcs, dsts, sems = refs[:4], refs[4:8], refs[8]
    copies = [pltpu.make_async_copy(a, b, sems.at[i]) for i, (a, b) in enumerate(zip(srcs, dsts))]
    for copy in copies:
        copy.start()
    for copy in copies:
        copy.wait()


def body(D, R, grads, master, first_moment, second_moment):
    rows, cols = grads.shape[1:]
    Z, n = D // 2, D * R
    t = rows // (D * R * 2)
    hbm = pl.BlockSpec(memory_space=pltpu.HBM)
    vmem = pl.BlockSpec(memory_space=pltpu.VMEM)
    bf16 = jnp.bfloat16
    part = (2, 2, 2, t, cols)
    dma = pltpu.SemaphoreType.DMA
    shapes = [((Z, 2) + part, bf16)] + [(part, F32)] * 3
    held_bytes = sum(math.prod(dims) * jnp.dtype(kind).itemsize for dims, kind in shapes)
    held = pl.pallas_call(
        functools.partial(kernel, Z, R, rows * cols),
        out_shape=[pltpu.VMEM(*shape) for shape in shapes],
        in_specs=[hbm] * 4,
        out_specs=[vmem] * 4,
        scratch_shapes=[
            pltpu.VMEM((Z,) + part, bf16),
            pltpu.VMEM((Z,) + part, bf16),
            pltpu.VMEM((Z,) + part, F32),
            pltpu.VMEM((Z, 2, t, cols), F32),
            pltpu.VMEM((Z, 2, t, cols), F32),
            pltpu.VMEM((Z, 2, t, cols), F32),
            pltpu.VMEM((Z - 1, 2, t, cols), F32),
            pltpu.VMEM(part, F32),
            pltpu.VMEM((n, 1, 128), F32),
            dma((2 * Z,)), dma((3,)),
            dma((2, 2 * Z)), dma((2, 2 * Z)), dma((2, 2 * Z)), dma((2, 2 * Z)), dma((2, 2 * Z)), dma((2, 2 * Z)),
            dma((2, n)), dma((2, 3)),
            dma((2, 2 * Z)), dma((2, 2 * Z)), dma((2, 2 * Z)), dma((2, 2 * Z)), dma((2, 2 * Z)), dma((2, 2 * Z)),
        ],
        compiler_params=pltpu.CompilerParams(
            collective_id=0, has_side_effects=True, vmem_limit_bytes=VMEM_BYTES - held_bytes
        ),
    )(
        grads.reshape((Z, 2) + part),
        master.reshape(part), first_moment.reshape(part), second_moment.reshape(part),
    )
    outs = pl.pallas_call(
        write_out,
        out_shape=[jax.ShapeDtypeStruct(*shape) for shape in shapes],
        in_specs=[vmem] * 4,
        out_specs=[hbm] * 4,
        scratch_shapes=[dma((4,))],
        compiler_params=pltpu.CompilerParams(vmem_limit_bytes=1024 * 1024),
    )(*held)
    weights, new_master, new_first, new_second = outs
    block = (rows // D, cols)
    return (weights.reshape(rows, cols), new_master.reshape(block), new_first.reshape(block), new_second.reshape(block))


def solution(mesh):
    D, R = mesh.shape["dp"], mesh.shape["rep"]
    assert R == 4 and D % 2 == 0
    in_specs = (P(("dp", "rep"), None, None), P("dp", None), P("dp", None), P("dp", None))
    out_specs = (P(), P("dp", None), P("dp", None), P("dp", None))
    return jax.shard_map(
        functools.partial(body, D, R), mesh=mesh, in_specs=in_specs, out_specs=out_specs, check_vma=False
    )
```
